32 devices in a mesh: fsdp: 16 (over z, x, core), tp: 2 (over y).
Axes of the slice: x: 2, y: 2, z: 4, core: 2. Of those that a mesh axis runs over, the one named last changes fastest.
Arguments:
- tokens: bfloat16 [2048, 3584], P('fsdp', 'tp'), may hold values from -6 to 6
- norm_gain: bfloat16 [3584], replicated, may hold values from 0.5 to 1.5
- gate_weight: bfloat16 [3584, 10240], P('fsdp', 'tp'), may hold values from -0.09375 to 0.09375
- up_weight: bfloat16 [3584, 10240], P('fsdp', 'tp'), may hold values from -0.09375 to 0.09375
- down_weight: bfloat16 [3584, 10240], P('fsdp', 'tp'), may hold values from -0.0625 to 0.0625
- probes: bfloat16 [2, 3584, 10240], P(None, 'fsdp', 'tp'), may hold values from -0.0625 to 0.0625
Outputs:
- layer_out: bfloat16 [2048, 3584], P('tp', 'fsdp')
- token_curv: float32 [2048], P('tp')
The draws below stay inside these ranges and needn't reach their ends.
All inputs are finite; a program needn't handle non-finite values.
Results may differ from the reference program's by a relative error of at most 0.014.
Values may be sent and summed in bfloat16 or wider, within the bound.
A program may use at most 128 MiB of HBM per device.

```python
import jax
import jax.numpy as jnp
from jax import lax

D = 3584
FF = 10240
PROBES = 2
TOKENS = 2048
N_TP = 2


def level_of(rng, dims, cuts, smallest, largest):
    def one(dim, parts):
        steps = jax.random.uniform(jax.random.fold_in(jax.random.fold_in(rng, 6), dim), (parts,), jnp.float32, smallest / len(cuts), largest / len(cuts))
        return jnp.repeat(jnp.exp(steps), dims[dim] // parts).reshape((-1,) + (1,) * (len(dims) - dim - 1))

    gain = one(*cuts[0])
    for cut in cuts[1:]:
        gain = gain * one(*cut)
    return gain


def bell_draw(own_key, dims, width, most, shards=(), dtype=jnp.bfloat16):
    factor_of = level_of(own_key, dims, shards, -0.22, 0.18) if shards else 1.0
    entries = jax.random.normal(own_key, dims, jnp.float32) * width * factor_of
    return jnp.minimum(jnp.maximum(entries, -most), most).astype(dtype)


def setup_inputs(seed: int = 0) -> dict:
    arg_keys = jax.random.split(jax.random.key(seed), 7)
    return {
        "tokens": bell_draw(arg_keys[0], (TOKENS, D), 1.0, 6.0, ((0, 16), (1, 2))),
        "norm_gain": jnp.clip(1.0 + 0.1 * jax.random.normal(arg_keys[1], (D,), jnp.float32), 0.5, 1.5).astype(jnp.bfloat16),
        "gate_weight": bell_draw(arg_keys[2], (D, FF), D ** -0.5, 0.09375, ((0, 16), (1, 2))),
        "up_weight": bell_draw(arg_keys[3], (D, FF), D ** -0.5, 0.09375, ((0, 16), (1, 2))),
        "down_weight": bell_draw(arg_keys[4], (D, FF), FF ** -0.5, 0.0625, ((0, 16), (1, 2))),
        "probes": bell_draw(arg_keys[5], (PROBES, D, FF), FF ** -0.5, 0.0625, ((1, 16), (2, 2))),
    }


epsilon = 1e-06

def reference(tokens, norm_gain, gate_weight, up_weight, down_weight, probes):
    widened = tokens.astype(jnp.float32)
    inverse_rms = lax.rsqrt(lax.optimization_barrier(jnp.mean(widened * widened, axis=1, keepdims=True)) + epsilon)
    normed = (widened * inverse_rms * norm_gain.astype(jnp.float32)).astype(jnp.bfloat16)
    gate_sum = jnp.dot(normed, gate_weight, preferred_element_type=jnp.float32)
    up_sum = jnp.dot(normed, up_weight, preferred_element_type=jnp.float32)
    hidden = (jax.nn.silu(gate_sum) * up_sum).astype(jnp.bfloat16)
    stacked = jnp.concatenate([down_weight[None], probes], axis=0)
    count = stacked.shape[0]
    block_width = FF // N_TP

    def add_block(block_index, running):
        offset = (block_index * block_width).astype(jnp.int32)
        columns = lax.dynamic_slice_in_dim(hidden, offset, block_width, 1)
        matrices = lax.dynamic_slice_in_dim(stacked, offset, block_width, 2)
        terms = [lax.dot_general(columns, matrices[which], (((1,), (1,)), ((), ())), preferred_element_type=jnp.float32).astype(jnp.bfloat16).astype(jnp.float32) for which in range(count)]
        return running + jnp.stack(terms)
    projected = lax.fori_loop(0, N_TP, add_block, jnp.zeros((count, TOKENS, D), jnp.float32))
    primal = projected[0]
    squashed = jax.nn.sigmoid(primal)
    slope = squashed * (1.0 - squashed)
    tangent_sq = lax.optimization_barrier(jnp.sum(projected[1:] * projected[1:], axis=0))
    token_curv = lax.optimization_barrier(jnp.sum(slope * tangent_sq, axis=1)) / (PROBES * D)
    return (primal.astype(jnp.bfloat16), token_curv)
```

```python
import jax
import jax.numpy as jnp
from jax import lax
from jax.experimental import pallas as pl
from jax.experimental.pallas import tpu as pltpu
from jax.sharding import PartitionSpec as P

D = 3584
PROBES = 2
MESH = pl.DeviceIdType.MESH
ANY = pl.BlockSpec(memory_space=pl.ANY)


epsilon = 1e-06


def remote(src, dst, send, recv, device):
    return pltpu.make_async_remote_copy(
        src_ref=src,
        dst_ref=dst,
        send_sem=send,
        recv_sem=recv,
        device_id=device,
        device_id_type=MESH,
    )


def fused_kernel(chips, t_ref, gain_ref, g_ref, u_ref, m0_ref, mp_ref, out_ref, curv_ref, tok, wts, hall, mats, acc, mine, theirs, other, curves,
                 t_send, t_recv, w_send, w_recv, wc_send, wc_recv, z_send, x_send, h_recv, c_send, c_recv, y_send, y_recv, v_send, v_recv, local_sem):
    me = lax.axis_index("fsdp")
    tp = lax.axis_index("tp")
    chip, core = me // 2, me % 2
    outer, inner = chip // 2, chip % 2
    outers = chips // 2
    devices = 2 * chips
    owners = chips // 2
    parts, t_rows, t_cols = t_ref.shape
    rows = g_ref.shape[0]
    count = hall.shape[0]
    width = hall.shape[-1]
    kinds, col_width = 1 + mp_ref.shape[0], m0_ref.shape[0]
    side_chip = outer * 2 + 1 - inner
    partner = {"fsdp": chip * 2 + 1 - core}
    across = {"tp": 1 - tp}
    down = {"fsdp": (chip - 2) * 2 + core}
    up = {"fsdp": (chip + 2) * 2 + core}
    side = {"fsdp": side_chip * 2 + core}
    features = chips * 2 * rows

    barrier = pltpu.get_barrier_semaphore()
    for d in range(1, devices):
        pl.semaphore_signal(barrier, inc=1, device_id={"fsdp": (me + d) % devices}, device_id_type=MESH)
    pl.semaphore_signal(barrier, inc=1, device_id=across, device_id_type=MESH)
    pl.semaphore_wait(barrier, devices)

    def token_slot(half, owner):
        return tok.at[owner, :, :, pl.ds(pl.multiple_of(half * t_cols, 128), t_cols)]

    def token_copy(src, half, owner, way, device):
        return remote(src, token_slot(half, owner), t_send.at[way, owner], t_recv.at[half, owner], device)

    def pass_on(src, owner, first):
        if first in (0, 1):
            @pl.when(outer > 0)
            def _():
                token_copy(src, tp, owner, 0, down).start()
        if first in (0, 2):
            @pl.when(outer < outers - 1)
            def _():
                token_copy(src, tp, owner, 1, up).start()
        token_copy(src, tp, owner, 2, side).start()
        token_copy(src, tp, owner, 3, across).start()

    def token_wait(half, owner):
        slot = token_slot(half, owner)
        remote(slot, slot, t_send.at[3, owner], t_recv.at[half, owner], across).wait_recv()

    weights = (g_ref, u_ref)

    def piece(a, owner):
        return weights[a].at[:, pl.ds(pl.multiple_of(owner * width, 128), width)]

    def landing(a, source, c):
        return wts.at[source, c, :, pl.ds(a * width, width)]

    def weight_send(a, peer):
        return remote(piece(a, peer), landing(a, chip, core), w_send.at[a, peer], w_recv.at[a, chip], {"fsdp": peer * 2 + core})

    def weight_pass(a, source):
        block = landing(a, source, core)
        return remote(block, block, wc_send.at[a, source], wc_recv.at[a, source], partner)

    def line(base, step, act):
        for d in range(outers - 1, 0, -1):
            @pl.when((outer + step * d >= 0) & (outer + step * d < outers))
            def _():
                for a in range(2):
                    act(a, base + 2 * step * d)

    def start_send(a, peer):
        weight_send(a, peer).start()

    def weights_along(r):
        @pl.when(outer == r)
        def _():
            line(chip, 1, start_send)

        @pl.when(outer == outers - 1 - r)
        def _():
            line(chip, -1, start_send)

    pass_on(t_ref, chip, 0)
    weights_along(0)
    own_out = [remote(piece(a, chip), landing(a, chip, core), wc_send.at[a, chip], wc_recv.at[a, chip], partner) for a in range(2)]
    locals_ = [pltpu.make_async_copy(piece(a, chip), landing(a, chip, core), local_sem.at[a]) for a in range(2)]
    locals_ += [
        pltpu.make_async_copy(t_ref, token_slot(tp, chip), local_sem.at[2]),
        pltpu.make_async_copy(m0_ref, mats.at[0], local_sem.at[3]),
        pltpu.make_async_copy(mp_ref, mats.at[pl.ds(1, kinds - 1)], local_sem.at[4]),
    ]
    for copy in own_out + locals_:
        copy.start()

    for r in range(1, outers):
        @pl.when(outer - r >= 0)
        def _():
            owner = chip - 2 * r
            token_wait(tp, owner)
            pass_on(token_slot(tp, owner), owner, 2)

        @pl.when(outer + r < outers)
        def _():
            owner = chip + 2 * r
            token_wait(tp, owner)
            pass_on(token_slot(tp, owner), owner, 1)

        weights_along(r)
    line(side_chip, 1, start_send)
    line(side_chip, -1, start_send)
    for a in range(2):
        start_send(a, side_chip)

    for z in range(outers):
        owner = z * 2 + 1 - inner
        token_wait(tp, owner)
        token_copy(token_slot(tp, owner), tp, owner, 3, across).start()

    def take(a, source):
        block = landing(a, source, core)
        remote(block, block, w_send.at[a, source], w_recv.at[a, source], partner).wait_recv()
        weight_pass(a, source).start()

    line(chip, 1, take)
    line(chip, -1, take)
    for a in range(2):
        take(a, side_chip)
    line(side_chip, 1, take)
    line(side_chip, -1, take)
    for s in range(chips):
        token_wait(1 - tp, s)
    for s in range(chips):
        for a in range(2):
            block = landing(a, s, 1 - core)
            remote(block, block, wc_send.at[a, s], wc_recv.at[a, s], partner).wait_recv()
    for copy in locals_:
        copy.wait()

    def hidden(k):
        o, s = k // parts, k % parts

        def normed(owner):
            widened = tok[owner, s].astype(jnp.float32)
            inverse_rms = lax.rsqrt(jnp.mean(widened * widened, axis=1, keepdims=True) + epsilon)
            return (widened * inverse_rms * gain_ref[...].astype(jnp.float32)).astype(jnp.bfloat16)

        left = jnp.concatenate([normed(o), normed(owners + o)], axis=0)
        sums = jnp.dot(left, wts[...].reshape(features, 2 * width), preferred_element_type=jnp.float32)
        values = (jax.nn.silu(sums[:, :width]) * sums[:, width:]).astype(jnp.bfloat16)
        hall[k, chip, core, 0] = values[:t_rows]
        hall[k, chip, core, 1] = values[t_rows:]

    def block_of(k, j):
        return hall.at[k, j, core]

    def along(k, j, way):
        block = block_of(k, j)
        return remote(block, block, z_send.at[way, k, j], h_recv.at[k, j], (down, up)[way])

    def sideways(k, j):
        block = block_of(k, j)
        return remote(block, block, x_send.at[k, j], h_recv.at[k, j], side)

    def relay(k, j):
        block = block_of(k, j)
        return remote(block, block, c_send.at[k, j], c_recv.at[k, j], partner)

    def arrived(k, j):
        sideways(k, j).wait_recv()

    def go(k, j, way):
        @pl.when((outer > 0) if way == 0 else (outer < outers - 1))
        def _():
            along(k, j, way).start()

    def doubled(k, z):
        return (k % 2 == 1) & ((z == 0) | (z == outers - 1))

    def inject(k):
        for way in range(2):
            go(k, chip, way)
        sideways(k, chip).start()
        relay(k, chip).start()

    def hop(k, r, way):
        z = outer - r if way else outer + r

        @pl.when((z >= 0) & (z < outers))
        def _():
            j = z * 2 + inner
            arrived(k, j)
            go(k, j, way)

            @pl.when(jnp.logical_not(doubled(k, z)))
            def _():
                sideways(k, j).start()

            relay(k, j).start()

    def beside(k, d):
        def one(z, way):
            @pl.when((z >= 0) & (z < outers))
            def _():
                j = z * 2 + 1 - inner
                arrived(k, j)
                if d == 0:
                    @pl.when(doubled(k, z))
                    def _():
                        for w in range(2):
                            go(k, j, w)
                else:
                    @pl.when(doubled(k, z))
                    def _():
                        go(k, j, way)

                relay(k, j).start()

        one(outer - d, 1)
        if d:
            one(outer + d, 0)

    def to_across(k):
        return remote(theirs.at[k], other.at[k], y_send.at[k], y_recv.at[k], across)

    def finish(k):
        for j in range(chips):
            block = hall.at[k, j, 1 - core]
            remote(block, block, c_send.at[k, j], c_recv.at[k, j], partner).wait_recv()
        acc[...] = jnp.zeros_like(acc)

        @pl.loop(0, chips // 2)
        def _(p):
            right = jnp.concatenate(
                [jnp.concatenate([hall[k, 2 * p, c, half], hall[k, 2 * p + 1, c, half]], axis=1) for half in range(2) for c in range(2)],
                axis=0,
            )
            left = mats[:, :, pl.ds(pl.multiple_of(p * 2 * width, 128), 2 * width)].reshape(kinds * col_width, 2 * width)
            acc[...] += lax.dot_general(left, right, (((1,), (1,)), ((), ())), preferred_element_type=jnp.float32)

        def lanes(half):
            return pl.ds(pl.multiple_of(half * 2 * t_rows, 128), 2 * t_rows)

        theirs[k] = acc[:, lanes(1 - tp)].astype(jnp.bfloat16)
        mine[k] = acc[:, lanes(tp)].astype(jnp.bfloat16)
        to_across(k).start()

    def conclude(k):
        to_across(k).wait_recv()

        def total(m):
            span = pl.ds(m * col_width, col_width)
            return mine[k, span, :].astype(jnp.float32) + other[k, span, :].astype(jnp.float32)

        primal = total(0)
        squashed = jax.nn.sigmoid(primal)
        squares = jnp.zeros_like(primal)
        for m in range(1, kinds):
            tangent = total(m)
            squares += tangent * tangent
        terms = squashed * (1.0 - squashed) * squares
        curves[me, pl.ds(k, 1), :] = jnp.sum(terms, axis=0, keepdims=True)
        fill = -col_width % 128
        turned = jnp.concatenate([primal, jnp.zeros((fill, 2 * t_rows), jnp.float32)], axis=0).T.astype(jnp.bfloat16)
        o, s = k // parts, k % parts
        for c in range(2):
            span = pl.ds(pl.multiple_of(((o * 2 + c) * parts + s) * t_rows, t_rows), t_rows)
            out_ref[span, :] = turned[c * t_rows : (c + 1) * t_rows, :col_width]

    lag = outers

    @pl.loop(0, count + lag)
    def _(i):
        @pl.when(i < count)
        def _():
            hidden(i)
            inject(i)

        for r in range(1, outers):
            @pl.when((i - r >= 0) & (i - r < count))
            def _():
                hop(i - r, r, 0)
                hop(i - r, r, 1)

        for d in range(outers):
            @pl.when((i - d - 1 >= 0) & (i - d - 1 < count))
            def _():
                beside(i - d - 1, d)

        @pl.when((i - lag >= 0) & (i - lag < count))
        def _():
            finish(i - lag)

        @pl.when((i - lag - 1 >= 0) & (i - lag - 1 < count))
        def _():
            conclude(i - lag - 1)

    conclude(count - 1)

    def curve(owner, d):
        return remote(curves.at[owner], curves.at[owner], v_send.at[d], v_recv.at[owner], {"fsdp": (me + d) % devices})

    for d in range(1, devices):
        curve(me, d).start()

    def drop(a, peer):
        weight_send(a, peer).wait_send()

    for base in (chip, side_chip):
        line(base, 1, drop)
        line(base, -1, drop)
    for a in range(2):
        drop(a, side_chip)
    for copy in own_out:
        copy.wait_send()
    for a in range(2):
        for s in range(chips):
            @pl.when(s != chip)
            def _():
                weight_pass(a, s).wait_send()

    def sent(owner, way):
        slot = token_slot(tp, owner)
        remote(slot, slot, t_send.at[way, owner], t_recv.at[tp, owner], across).wait_send()

    for s in range(chips):
        sent(s, 3)
    for r in range(outers):
        @pl.when(outer - r >= 0)
        def _():
            owner = chip - 2 * r
            sent(owner, 2)

            @pl.when(outer < outers - 1)
            def _():
                sent(owner, 1)

        @pl.when(outer + r < outers)
        def _():
            owner = chip + 2 * r
            if r > 0:
                sent(owner, 2)

            @pl.when(outer > 0)
            def _():
                sent(owner, 0)

    @pl.loop(0, count)
    def _(k):
        to_across(k).wait_send()
        for j in range(chips):
            relay(k, j).wait_send()
        for z in range(outers):
            j = z * 2 + inner
            twin = z * 2 + 1 - inner
            twice = doubled(k, z)

            @pl.when((z == outer) | jnp.logical_not(twice))
            def _():
                sideways(k, j).wait_send()

            def went(way):
                along(k, j, way).wait_send()

                @pl.when(twice)
                def _():
                    along(k, twin, way).wait_send()

            @pl.when((outer <= z) & (outer > 0))
            def _():
                went(0)

            @pl.when((outer >= z) & (outer < outers - 1))
            def _():
                went(1)

    for d in range(1, devices):
        curve((me + devices - d) % devices, d).wait_recv()
        curve(me, d).wait_send()
    curv_ref[...] = jnp.sum(curves[...], axis=0) / (PROBES * D)


def fused(tokens, norm_gain, gate_weight, up_weight, down_weight, probes, chips):
    t_all, t_cols = tokens.shape
    parts = 2 if t_all % 128 == 0 else 1
    t_rows = t_all // parts
    rows, columns = gate_weight.shape
    width = columns // chips
    col_width, span = down_weight.shape
    kinds = 1 + probes.shape[0]
    count = parts * chips // 2
    kept = count * 2 * t_rows
    pieces = pltpu.SemaphoreType.DMA((2, chips))
    hops = pltpu.SemaphoreType.DMA((count, chips))
    part = pltpu.VMEM((count, kinds * col_width, 2 * t_rows), jnp.bfloat16)
    vmem = pl.BlockSpec(memory_space=pltpu.VMEM)
    out, curv = pl.pallas_call(
        lambda *refs: fused_kernel(chips, *refs),
        out_shape=(jax.ShapeDtypeStruct((kept, col_width), jnp.bfloat16), jax.ShapeDtypeStruct((count, 2 * t_rows), jnp.float32)),
        in_specs=[ANY, vmem, ANY, ANY, ANY, ANY],
        out_specs=[vmem] * 2,
        scratch_shapes=[
            pltpu.VMEM((chips, parts, t_rows, 2 * t_cols), jnp.bfloat16),
            pltpu.VMEM((chips, 2, rows, 2 * width), jnp.bfloat16),
            pltpu.VMEM((count, chips, 2, 2, t_rows, width), jnp.bfloat16),
            pltpu.VMEM((kinds, col_width, span), jnp.bfloat16),
            pltpu.VMEM((kinds * col_width, 4 * t_rows), jnp.float32),
            part,
            part,
            part,
            pltpu.VMEM((2 * chips, count, 2 * t_rows), jnp.float32),
            pltpu.SemaphoreType.DMA((4, chips)),
            pieces,
            pieces,
            pieces,
            pieces,
            pieces,
            pltpu.SemaphoreType.DMA((2, count, chips)),
            hops,
            hops,
            hops,
            hops,
            pltpu.SemaphoreType.DMA((count,)),
            pltpu.SemaphoreType.DMA((count,)),
            pltpu.SemaphoreType.DMA((2 * chips,)),
            pltpu.SemaphoreType.DMA((2 * chips,)),
            pltpu.SemaphoreType.DMA((5,)),
        ],
        compiler_params=pltpu.CompilerParams(collective_id=1, has_side_effects=True, vmem_limit_bytes=63 * 2**20),
        name="fused",
    )(tokens.reshape(parts, t_rows, t_cols), norm_gain.reshape(1, -1), gate_weight, up_weight, down_weight, probes)
    curv = curv.reshape(count // parts, parts, 2, t_rows).transpose(0, 2, 1, 3)
    return out, curv.reshape(kept)


def norm(features, norm_gain):
    widened = features.astype(jnp.float32)
    inverse_rms = lax.rsqrt(jnp.mean(widened * widened, axis=1, keepdims=True) + epsilon)
    return (widened * inverse_rms * norm_gain.astype(jnp.float32)).astype(jnp.bfloat16)


def dot(a, b):
    return jnp.dot(a, b, preferred_element_type=jnp.float32)


def project(hidden_all, down_weight, probes):
    stacked = jnp.concatenate([down_weight[None], probes], axis=0)
    count = stacked.shape[0]
    col_width = stacked.shape[1]
    flat_weights = stacked.reshape(count * col_width, stacked.shape[2])
    partial_terms = lax.dot_general(
        hidden_all,
        flat_weights,
        (((1,), (1,)), ((), ())),
        preferred_element_type=jnp.float32,
    )
    summed = lax.psum_scatter(
        partial_terms.astype(jnp.bfloat16), "tp", scatter_dimension=0, tiled=True
    ).astype(jnp.float32)
    summed_parts = summed.reshape(summed.shape[0], count, col_width)
    primal = summed_parts[:, 0, :]
    tangents = summed_parts[:, 1:, :]
    squashed = jax.nn.sigmoid(primal)
    slope = squashed * (1.0 - squashed)
    tangent_sq = jnp.sum(tangents * tangents, axis=1)
    local_curv = jnp.sum(slope * tangent_sq, axis=1) / (PROBES * D)
    token_curv = lax.psum(local_curv, "fsdp")
    return (primal.astype(jnp.bfloat16), token_curv)


def gathered_weights(tokens, norm_gain, gate_weight, up_weight, down_weight, probes):
    normed = norm(lax.all_gather(tokens, "tp", axis=1, tiled=True), norm_gain)
    gate_sum = dot(normed, lax.all_gather(gate_weight, "fsdp", axis=0, tiled=True))
    up_sum = dot(normed, lax.all_gather(up_weight, "fsdp", axis=0, tiled=True))
    hidden = (jax.nn.silu(gate_sum) * up_sum).astype(jnp.bfloat16)
    return project(lax.all_gather(hidden, "fsdp", axis=0, tiled=True), down_weight, probes)


def moved_weights(tokens, norm_gain, gate_weight, up_weight, down_weight, probes):
    chips = lax.axis_size("fsdp") // 2
    return fused(tokens, norm_gain, gate_weight, up_weight, down_weight, probes, chips)


def solution(mesh):
    def on_device(tokens, norm_gain, gate_weight, up_weight, down_weight, probes):
        chips = mesh.shape["fsdp"] // 2
        fits = mesh.shape["tp"] == 2 and chips % 2 == 0 and gate_weight.shape[1] % (128 * chips) == 0 and tokens.shape[1] % 128 == 0
        form = moved_weights if fits else gathered_weights
        return form(tokens, norm_gain, gate_weight, up_weight, down_weight, probes)

    return jax.shard_map(
        on_device,
        mesh=mesh,
        in_specs=(
            P("fsdp", "tp"),
            P(),
            P("fsdp", "tp"),
            P("fsdp", "tp"),
            P("fsdp", "tp"),
            P(None, "fsdp", "tp"),
        ),
        out_specs=(P("tp", "fsdp"), P("tp")),
        check_vma=False,
    )
```

```python
import jax
import jax.numpy as jnp
from jax import lax
from jax.experimental import pallas as pl
from jax.experimental.pallas import tpu as pltpu
from jax.sharding import PartitionSpec as P

D = 3584
PROBES = 2
MESH = pl.DeviceIdType.MESH
ANY = pl.BlockSpec(memory_space=pl.ANY)


epsilon = 1e-06


def remote(src, dst, send, recv, device):
    return pltpu.make_async_remote_copy(
        src_ref=src,
        dst_ref=dst,
        send_sem=send,
        recv_sem=recv,
        device_id=device,
        device_id_type=MESH,
    )


def fused_kernel(chips, t_ref, gain_ref, g_ref, u_ref, m0_ref, mp_ref, out_ref, curv_ref, tok, wts, hall, mats, acc, mine, theirs, other, curves,
                 t_send, t_recv, w_send, w_recv, wc_send, wc_recv, z_send, x_send, h_recv, c_send, c_recv, y_send, y_recv, v_send, v_recv, local_sem):
    me = lax.axis_index("fsdp")
    tp = lax.axis_index("tp")
    chip, core = me // 2, me % 2
    outer, inner = chip // 2, chip % 2
    outers = chips // 2
    devices = 2 * chips
    owners = chips // 2
    parts, t_rows, t_cols = t_ref.shape
    rows = g_ref.shape[0]
    count = hall.shape[0]
    width = hall.shape[-1]
    kinds, col_width = 1 + mp_ref.shape[0], m0_ref.shape[0]
    side_chip = outer * 2 + 1 - inner
    partner = {"fsdp": chip * 2 + 1 - core}
    across = {"tp": 1 - tp}
    down = {"fsdp": (chip - 2) * 2 + core}
    up = {"fsdp": (chip + 2) * 2 + core}
    side = {"fsdp": side_chip * 2 + core}
    features = chips * 2 * rows

    barrier = pltpu.get_barrier_semaphore()
    for d in range(1, devices):
        pl.semaphore_signal(barrier, inc=1, device_id={"fsdp": (me + d) % devices}, device_id_type=MESH)
    pl.semaphore_signal(barrier, inc=1, device_id=across, device_id_type=MESH)
    pl.semaphore_wait(barrier, devices)

    def token_slot(half, owner):
        return tok.at[owner, :, :, pl.ds(pl.multiple_of(half * t_cols, 128), t_cols)]

    def token_copy(src, half, owner, way, device):
        return remote(src, token_slot(half, owner), t_send.at[way, owner], t_recv.at[half, owner], device)

    def pass_on(src, owner, first):
        if first in (0, 1):
            @pl.when(outer > 0)
            def _():
                token_copy(src, tp, owner, 0, down).start()
        if first in (0, 2):
            @pl.when(outer < outers - 1)
            def _():
                token_copy(src, tp, owner, 1, up).start()
        token_copy(src, tp, owner, 2, side).start()
        token_copy(src, tp, owner, 3, across).start()

    def token_wait(half, owner):
        slot = token_slot(half, owner)
        remote(slot, slot, t_send.at[3, owner], t_recv.at[half, owner], across).wait_recv()

    weights = (g_ref, u_ref)

    def piece(a, owner):
        return weights[a].at[:, pl.ds(pl.multiple_of(owner * width, 128), width)]

    def landing(a, source, c):
        return wts.at[source, c, :, pl.ds(a * width, width)]

    def weight_send(a, peer):
        return remote(piece(a, peer), landing(a, chip, core), w_send.at[a, peer], w_recv.at[a, chip], {"fsdp": peer * 2 + core})

    def weight_pass(a, source):
        block = landing(a, source, core)
        return remote(block, block, wc_send.at[a, source], wc_recv.at[a, source], partner)

    def line(base, step, act):
        for d in range(outers - 1, 0, -1):
            @pl.when((outer + step * d >= 0) & (outer + step * d < outers))
            def _():
                for a in range(2):
                    act(a, base + 2 * step * d)

    def start_send(a, peer):
        weight_send(a, peer).start()

    def weights_along(r):
        @pl.when(outer == r)
        def _():
            line(chip, 1, start_send)
            line(side_chip, 1, start_send)

        @pl.when(outer == outers - 1 - r)
        def _():
            line(chip, -1, start_send)
            line(side_chip, -1, start_send)

    pass_on(t_ref, chip, 0)
    for a in range(2):
        start_send(a, side_chip)
    weights_along(0)
    own_out = [remote(piece(a, chip), landing(a, chip, core), wc_send.at[a, chip], wc_recv.at[a, chip], partner) for a in range(2)]
    locals_ = [pltpu.make_async_copy(piece(a, chip), landing(a, chip, core), local_sem.at[a]) for a in range(2)]
    locals_ += [
        pltpu.make_async_copy(t_ref, token_slot(tp, chip), local_sem.at[2]),
        pltpu.make_async_copy(m0_ref, mats.at[0], local_sem.at[3]),
        pltpu.make_async_copy(mp_ref, mats.at[pl.ds(1, kinds - 1)], local_sem.at[4]),
    ]
    for copy in own_out + locals_:
        copy.start()

    for r in range(1, outers):
        @pl.when(outer - r >= 0)
        def _():
            owner = chip - 2 * r
            token_wait(tp, owner)
            pass_on(token_slot(tp, owner), owner, 2)

        @pl.when(outer + r < outers)
        def _():
            owner = chip + 2 * r
            token_wait(tp, owner)
            pass_on(token_slot(tp, owner), owner, 1)

        weights_along(r)

    for z in range(outers):
        owner = z * 2 + 1 - inner
        token_wait(tp, owner)
        token_copy(token_slot(tp, owner), tp, owner, 3, across).start()

    def take(a, source):
        block = landing(a, source, core)
        remote(block, block, w_send.at[a, source], w_recv.at[a, source], partner).wait_recv()
        weight_pass(a, source).start()

    line(chip, 1, take)
    line(chip, -1, take)
    for a in range(2):
        take(a, side_chip)
    line(side_chip, 1, take)
    line(side_chip, -1, take)
    for s in range(chips):
        for a in range(2):
            block = landing(a, s, 1 - core)
            remote(block, block, wc_send.at[a, s], wc_recv.at[a, s], partner).wait_recv()
    for copy in locals_:
        copy.wait()

    def hidden(k):
        o, s = k // parts, k % parts

        @pl.when(s == 0)
        def _():
            token_wait(1 - tp, o)
            token_wait(1 - tp, owners + o)

        def normed(owner):
            widened = tok[owner, s].astype(jnp.float32)
            inverse_rms = lax.rsqrt(jnp.mean(widened * widened, axis=1, keepdims=True) + epsilon)
            return (widened * inverse_rms * gain_ref[...].astype(jnp.float32)).astype(jnp.bfloat16)

        left = jnp.concatenate([normed(o), normed(owners + o)], axis=0)
        sums = jnp.dot(left, wts[...].reshape(features, 2 * width), preferred_element_type=jnp.float32)
        values = (jax.nn.silu(sums[:, :width]) * sums[:, width:]).astype(jnp.bfloat16)
        hall[k, chip, core, 0] = values[:t_rows]
        hall[k, chip, core, 1] = values[t_rows:]

    def block_of(k, j):
        return hall.at[k, j, core]

    def along(k, j, way):
        block = block_of(k, j)
        return remote(block, block, z_send.at[way, k, j], h_recv.at[k, j], (down, up)[way])

    def sideways(k, j):
        block = block_of(k, j)
        return remote(block, block, x_send.at[k, j], h_recv.at[k, j], side)

    def relay(k, j):
        block = block_of(k, j)
        return remote(block, block, c_send.at[k, j], c_recv.at[k, j], partner)

    def arrived(k, j):
        sideways(k, j).wait_recv()

    def go(k, j, way):
        @pl.when((outer > 0) if way == 0 else (outer < outers - 1))
        def _():
            along(k, j, way).start()

    def doubled(k, z):
        return (k % 2 == 1) & ((z == 0) | (z == outers - 1))

    def inject(k):
        for way in range(2):
            go(k, chip, way)
        sideways(k, chip).start()
        relay(k, chip).start()

    def hop(k, r, way):
        z = outer - r if way else outer + r

        @pl.when((z >= 0) & (z < outers))
        def _():
            j = z * 2 + inner
            arrived(k, j)
            go(k, j, way)

            @pl.when(jnp.logical_not(doubled(k, z)))
            def _():
                sideways(k, j).start()

            relay(k, j).start()

    def beside(k, d):
        def one(z, way):
            @pl.when((z >= 0) & (z < outers))
            def _():
                j = z * 2 + 1 - inner
                arrived(k, j)
                if d == 0:
                    @pl.when(doubled(k, z))
                    def _():
                        for w in range(2):
                            go(k, j, w)
                else:
                    @pl.when(doubled(k, z))
                    def _():
                        go(k, j, way)

                relay(k, j).start()

        one(outer - d, 1)
        if d:
            one(outer + d, 0)

    def to_across(k):
        return remote(theirs.at[k], other.at[k], y_send.at[k], y_recv.at[k], across)

    def finish(k):
        for j in range(chips):
            block = hall.at[k, j, 1 - core]
            remote(block, block, c_send.at[k, j], c_recv.at[k, j], partner).wait_recv()
        acc[...] = jnp.zeros_like(acc)

        @pl.loop(0, chips // 2)
        def _(p):
            right = jnp.concatenate(
                [jnp.concatenate([hall[k, 2 * p, c, half], hall[k, 2 * p + 1, c, half]], axis=1) for half in range(2) for c in range(2)],
                axis=0,
            )
            left = mats[:, :, pl.ds(pl.multiple_of(p * 2 * width, 128), 2 * width)].reshape(kinds * col_width, 2 * width)
            acc[...] += lax.dot_general(left, right, (((1,), (1,)), ((), ())), preferred_element_type=jnp.float32)

        def lanes(half):
            return pl.ds(pl.multiple_of(half * 2 * t_rows, 128), 2 * t_rows)

        theirs[k] = acc[:, lanes(1 - tp)].astype(jnp.bfloat16)
        mine[k] = acc[:, lanes(tp)].astype(jnp.bfloat16)
        to_across(k).start()

    def conclude(k):
        to_across(k).wait_recv()

        def total(m):
            span = pl.ds(m * col_width, col_width)
            return mine[k, span, :].astype(jnp.float32) + other[k, span, :].astype(jnp.float32)

        primal = total(0)
        squashed = jax.nn.sigmoid(primal)
        squares = jnp.zeros_like(primal)
        for m in range(1, kinds):
            tangent = total(m)
            squares += tangent * tangent
        terms = squashed * (1.0 - squashed) * squares
        curves[me, pl.ds(k, 1), :] = jnp.sum(terms, axis=0, keepdims=True)
        fill = -col_width % 128
        turned = jnp.concatenate([primal, jnp.zeros((fill, 2 * t_rows), jnp.float32)], axis=0).T.astype(jnp.bfloat16)
        o, s = k // parts, k % parts
        for c in range(2):
            span = pl.ds(pl.multiple_of(((o * 2 + c) * parts + s) * t_rows, t_rows), t_rows)
            out_ref[span, :] = turned[c * t_rows : (c + 1) * t_rows, :col_width]

    lag = outers

    @pl.loop(0, count + lag)
    def _(i):
        @pl.when(i < count)
        def _():
            hidden(i)
            inject(i)

        for r in range(1, outers):
            @pl.when((i - r >= 0) & (i - r < count))
            def _():
                hop(i - r, r, 0)
                hop(i - r, r, 1)

        for d in range(outers):
            @pl.when((i - d - 1 >= 0) & (i - d - 1 < count))
            def _():
                beside(i - d - 1, d)

        @pl.when((i - lag >= 0) & (i - lag < count))
        def _():
            finish(i - lag)

        @pl.when((i - lag - 1 >= 0) & (i - lag - 1 < count))
        def _():
            conclude(i - lag - 1)

    conclude(count - 1)

    def curve(owner, d):
        return remote(curves.at[owner], curves.at[owner], v_send.at[d], v_recv.at[owner], {"fsdp": (me + d) % devices})

    for d in range(1, devices):
        curve(me, d).start()

    def drop(a, peer):
        weight_send(a, peer).wait_send()

    for base in (chip, side_chip):
        line(base, 1, drop)
        line(base, -1, drop)
    for a in range(2):
        drop(a, side_chip)
    for copy in own_out:
        copy.wait_send()
    for a in range(2):
        for s in range(chips):
            @pl.when(s != chip)
            def _():
                weight_pass(a, s).wait_send()

    def sent(owner, way):
        slot = token_slot(tp, owner)
        remote(slot, slot, t_send.at[way, owner], t_recv.at[tp, owner], across).wait_send()

    for s in range(chips):
        sent(s, 3)
    for r in range(outers):
        @pl.when(outer - r >= 0)
        def _():
            owner = chip - 2 * r
            sent(owner, 2)

            @pl.when(outer < outers - 1)
            def _():
                sent(owner, 1)

        @pl.when(outer + r < outers)
        def _():
            owner = chip + 2 * r
            if r > 0:
                sent(owner, 2)

            @pl.when(outer > 0)
            def _():
                sent(owner, 0)

    @pl.loop(0, count)
    def _(k):
        to_across(k).wait_send()
        for j in range(chips):
            relay(k, j).wait_send()
        for z in range(outers):
            j = z * 2 + inner
            twin = z * 2 + 1 - inner
            twice = doubled(k, z)

            @pl.when((z == outer) | jnp.logical_not(twice))
            def _():
                sideways(k, j).wait_send()

            def went(way):
                along(k, j, way).wait_send()

                @pl.when(twice)
                def _():
                    along(k, twin, way).wait_send()

            @pl.when((outer <= z) & (outer > 0))
            def _():
                went(0)

            @pl.when((outer >= z) & (outer < outers - 1))
            def _():
                went(1)

    for d in range(1, devices):
        curve((me + devices - d) % devices, d).wait_recv()
        curve(me, d).wait_send()
    curv_ref[...] = jnp.sum(curves[...], axis=0) / (PROBES * D)


def fused(tokens, norm_gain, gate_weight, up_weight, down_weight, probes, chips):
    t_all, t_cols = tokens.shape
    parts = 2 if t_all % 128 == 0 else 1
    t_rows = t_all // parts
    rows, columns = gate_weight.shape
    width = columns // chips
    col_width, span = down_weight.shape
    kinds = 1 + probes.shape[0]
    count = parts * chips // 2
    kept = count * 2 * t_rows
    pieces = pltpu.SemaphoreType.DMA((2, chips))
    hops = pltpu.SemaphoreType.DMA((count, chips))
    part = pltpu.VMEM((count, kinds * col_width, 2 * t_rows), jnp.bfloat16)
    vmem = pl.BlockSpec(memory_space=pltpu.VMEM)
    out, curv = pl.pallas_call(
        lambda *refs: fused_kernel(chips, *refs),
        out_shape=(jax.ShapeDtypeStruct((kept, col_width), jnp.bfloat16), jax.ShapeDtypeStruct((count, 2 * t_rows), jnp.float32)),
        in_specs=[ANY, vmem, ANY, ANY, ANY, ANY],
        out_specs=[vmem] * 2,
        scratch_shapes=[
            pltpu.VMEM((chips, parts, t_rows, 2 * t_cols), jnp.bfloat16),
            pltpu.VMEM((chips, 2, rows, 2 * width), jnp.bfloat16),
            pltpu.VMEM((count, chips, 2, 2, t_rows, width), jnp.bfloat16),
            pltpu.VMEM((kinds, col_width, span), jnp.bfloat16),
            pltpu.VMEM((kinds * col_width, 4 * t_rows), jnp.float32),
            part,
            part,
            part,
            pltpu.VMEM((2 * chips, count, 2 * t_rows), jnp.float32),
            pltpu.SemaphoreType.DMA((4, chips)),
            pieces,
            pieces,
            pieces,
            pieces,
            pieces,
            pltpu.SemaphoreType.DMA((2, count, chips)),
            hops,
            hops,
            hops,
            hops,
            pltpu.SemaphoreType.DMA((count,)),
            pltpu.SemaphoreType.DMA((count,)),
            pltpu.SemaphoreType.DMA((2 * chips,)),
            pltpu.SemaphoreType.DMA((2 * chips,)),
            pltpu.SemaphoreType.DMA((5,)),
        ],
        compiler_params=pltpu.CompilerParams(collective_id=1, has_side_effects=True, vmem_limit_bytes=63 * 2**20),
        name="fused",
    )(tokens.reshape(parts, t_rows, t_cols), norm_gain.reshape(1, -1), gate_weight, up_weight, down_weight, probes)
    curv = curv.reshape(count // parts, parts, 2, t_rows).transpose(0, 2, 1, 3)
    return out, curv.reshape(kept)


def norm(features, norm_gain):
    widened = features.astype(jnp.float32)
    inverse_rms = lax.rsqrt(jnp.mean(widened * widened, axis=1, keepdims=True) + epsilon)
    return (widened * inverse_rms * norm_gain.astype(jnp.float32)).astype(jnp.bfloat16)


def dot(a, b):
    return jnp.dot(a, b, preferred_element_type=jnp.float32)


def project(hidden_all, down_weight, probes):
    stacked = jnp.concatenate([down_weight[None], probes], axis=0)
    count = stacked.shape[0]
    col_width = stacked.shape[1]
    flat_weights = stacked.reshape(count * col_width, stacked.shape[2])
    partial_terms = lax.dot_general(
        hidden_all,
        flat_weights,
        (((1,), (1,)), ((), ())),
        preferred_element_type=jnp.float32,
    )
    summed = lax.psum_scatter(
        partial_terms.astype(jnp.bfloat16), "tp", scatter_dimension=0, tiled=True
    ).astype(jnp.float32)
    summed_parts = summed.reshape(summed.shape[0], count, col_width)
    primal = summed_parts[:, 0, :]
    tangents = summed_parts[:, 1:, :]
    squashed = jax.nn.sigmoid(primal)
    slope = squashed * (1.0 - squashed)
    tangent_sq = jnp.sum(tangents * tangents, axis=1)
    local_curv = jnp.sum(slope * tangent_sq, axis=1) / (PROBES * D)
    token_curv = lax.psum(local_curv, "fsdp")
    return (primal.astype(jnp.bfloat16), token_curv)


def gathered_weights(tokens, norm_gain, gate_weight, up_weight, down_weight, probes):
    normed = norm(lax.all_gather(tokens, "tp", axis=1, tiled=True), norm_gain)
    gate_sum = dot(normed, lax.all_gather(gate_weight, "fsdp", axis=0, tiled=True))
    up_sum = dot(normed, lax.all_gather(up_weight, "fsdp", axis=0, tiled=True))
    hidden = (jax.nn.silu(gate_sum) * up_sum).astype(jnp.bfloat16)
    return project(lax.all_gather(hidden, "fsdp", axis=0, tiled=True), down_weight, probes)


def moved_weights(tokens, norm_gain, gate_weight, up_weight, down_weight, probes):
    chips = lax.axis_size("fsdp") // 2
    return fused(tokens, norm_gain, gate_weight, up_weight, down_weight, probes, chips)


def solution(mesh):
    def on_device(tokens, norm_gain, gate_weight, up_weight, down_weight, probes):
        chips = mesh.shape["fsdp"] // 2
        fits = mesh.shape["tp"] == 2 and chips % 2 == 0 and gate_weight.shape[1] % (128 * chips) == 0 and tokens.shape[1] % 128 == 0
        form = moved_weights if fits else gathered_weights
        return form(tokens, norm_gain, gate_weight, up_weight, down_weight, probes)

    return jax.shard_map(
        on_device,
        mesh=mesh,
        in_specs=(
            P("fsdp", "tp"),
            P(),
            P("fsdp", "tp"),
            P("fsdp", "tp"),
            P("fsdp", "tp"),
            P(None, "fsdp", "tp"),
        ),
        out_specs=(P("tp", "fsdp"), P("tp")),
        check_vma=False,
    )
```

```python
import jax
import jax.numpy as jnp
from jax import lax
from jax.experimental import pallas as pl
from jax.experimental.pallas import tpu as pltpu
from jax.sharding import PartitionSpec as P

D = 3584
PROBES = 2
MESH = pl.DeviceIdType.MESH
ANY = pl.BlockSpec(memory_space=pl.ANY)


epsilon = 1e-06


def remote(src, dst, send, recv, device):
    return pltpu.make_async_remote_copy(
        src_ref=src,
        dst_ref=dst,
        send_sem=send,
        recv_sem=recv,
        device_id=device,
        device_id_type=MESH,
    )


def fused_kernel(chips, t_ref, gain_ref, g_ref, u_ref, m0_ref, mp_ref, out_ref, curv_ref, tok, wts, hall, mats, acc, mine, theirs, other, curves,
                 t_send, t_recv, w_send, w_recv, wc_send, wc_recv, z_send, x_send, h_recv, c_send, c_recv, y_send, y_recv, v_send, v_recv, local_sem):
    me = lax.axis_index("fsdp")
    tp = lax.axis_index("tp")
    chip, core = me // 2, me % 2
    outer, inner = chip // 2, chip % 2
    outers = chips // 2
    devices = 2 * chips
    owners = chips // 2
    parts, t_rows, t_cols = t_ref.shape
    rows = g_ref.shape[0]
    count = hall.shape[0]
    width = hall.shape[-1]
    kinds, col_width = 1 + mp_ref.shape[0], m0_ref.shape[0]
    side_chip = outer * 2 + 1 - inner
    partner = {"fsdp": chip * 2 + 1 - core}
    across = {"tp": 1 - tp}
    down = {"fsdp": (chip - 2) * 2 + core}
    up = {"fsdp": (chip + 2) * 2 + core}
    side = {"fsdp": side_chip * 2 + core}
    features = chips * 2 * rows

    barrier = pltpu.get_barrier_semaphore()
    for d in range(1, devices):
        pl.semaphore_signal(barrier, inc=1, device_id={"fsdp": (me + d) % devices}, device_id_type=MESH)
    pl.semaphore_signal(barrier, inc=1, device_id=across, device_id_type=MESH)
    pl.semaphore_wait(barrier, devices)

    def token_slot(half, owner, part):
        return tok.at[owner, part, :, pl.ds(pl.multiple_of(half * t_cols, 128), t_cols)]

    def token_copy(src, half, owner, part, way, device):
        return remote(src, token_slot(half, owner, part), t_send.at[way, owner, part], t_recv.at[half, owner, part], device)

    def pass_on(src, owner, part, first):
        if first in (0, 1):
            @pl.when(outer > 0)
            def _():
                token_copy(src, tp, owner, part, 0, down).start()
        if first in (0, 2):
            @pl.when(outer < outers - 1)
            def _():
                token_copy(src, tp, owner, part, 1, up).start()
        token_copy(src, tp, owner, part, 2, side).start()
        token_copy(src, tp, owner, part, 3, across).start()

    def token_wait(half, owner, part):
        slot = token_slot(half, owner, part)
        remote(slot, slot, t_send.at[3, owner, part], t_recv.at[half, owner, part], across).wait_recv()

    weights = (g_ref, u_ref)

    def piece(a, owner):
        return weights[a].at[:, pl.ds(pl.multiple_of(owner * width, 128), width)]

    def landing(a, source, c):
        return wts.at[source, c, :, pl.ds(a * width, width)]

    def weight_send(a, peer):
        return remote(piece(a, peer), landing(a, chip, core), w_send.at[a, peer], w_recv.at[a, chip], {"fsdp": peer * 2 + core})

    def weight_pass(a, source):
        block = landing(a, source, core)
        return remote(block, block, wc_send.at[a, source], wc_recv.at[a, source], partner)

    def line(base, step, act):
        for d in range(outers - 1, 0, -1):
            @pl.when((outer + step * d >= 0) & (outer + step * d < outers))
            def _():
                for a in range(2):
                    act(a, base + 2 * step * d)

    def start_send(a, peer):
        weight_send(a, peer).start()

    def weights_along(r):
        @pl.when(outer == r)
        def _():
            line(chip, 1, start_send)
            line(side_chip, 1, start_send)

        @pl.when(outer == outers - 1 - r)
        def _():
            line(chip, -1, start_send)
            line(side_chip, -1, start_send)

    for part in range(parts):
        pass_on(t_ref.at[part], chip, part, 0)
    for a in range(2):
        start_send(a, side_chip)
    weights_along(0)
    own_out = [remote(piece(a, chip), landing(a, chip, core), wc_send.at[a, chip], wc_recv.at[a, chip], partner) for a in range(2)]
    locals_ = [pltpu.make_async_copy(piece(a, chip), landing(a, chip, core), local_sem.at[a]) for a in range(2)]
    locals_ += [
        pltpu.make_async_copy(t_ref, tok.at[chip, :, :, pl.ds(pl.multiple_of(tp * t_cols, 128), t_cols)], local_sem.at[2]),
        pltpu.make_async_copy(m0_ref, mats.at[0], local_sem.at[3]),
        pltpu.make_async_copy(mp_ref, mats.at[pl.ds(1, kinds - 1)], local_sem.at[4]),
    ]
    for copy in own_out + locals_:
        copy.start()

    for r in range(1, outers):
        @pl.when(outer - r >= 0)
        def _():
            owner = chip - 2 * r
            for part in range(parts):
                token_wait(tp, owner, part)
                pass_on(token_slot(tp, owner, part), owner, part, 2)

        @pl.when(outer + r < outers)
        def _():
            owner = chip + 2 * r
            for part in range(parts):
                token_wait(tp, owner, part)
                pass_on(token_slot(tp, owner, part), owner, part, 1)

        weights_along(r)

    for z in range(outers):
        owner = z * 2 + 1 - inner
        for part in range(parts):
            token_wait(tp, owner, part)
            token_copy(token_slot(tp, owner, part), tp, owner, part, 3, across).start()

    def take(a, source):
        block = landing(a, source, core)
        remote(block, block, w_send.at[a, source], w_recv.at[a, source], partner).wait_recv()
        weight_pass(a, source).start()

    line(chip, 1, take)
    line(chip, -1, take)
    for a in range(2):
        take(a, side_chip)
    line(side_chip, 1, take)
    line(side_chip, -1, take)
    for s in range(chips):
        for a in range(2):
            block = landing(a, s, 1 - core)
            remote(block, block, wc_send.at[a, s], wc_recv.at[a, s], partner).wait_recv()
    for copy in locals_:
        copy.wait()

    def hidden(k):
        o, s = k // parts, k % parts

        for half in range(2):
            token_wait(1 - tp, half * owners + o, s)

        def normed(owner):
            widened = tok[owner, s].astype(jnp.float32)
            inverse_rms = lax.rsqrt(jnp.mean(widened * widened, axis=1, keepdims=True) + epsilon)
            return (widened * inverse_rms * gain_ref[...].astype(jnp.float32)[None, :]).astype(jnp.bfloat16)

        left = jnp.concatenate([normed(o), normed(owners + o)], axis=0)
        sums = jnp.dot(left, wts[...].reshape(features, 2 * width), preferred_element_type=jnp.float32)
        values = (jax.nn.silu(sums[:, :width]) * sums[:, width:]).astype(jnp.bfloat16)
        hall[k, chip, core, 0] = values[:t_rows]
        hall[k, chip, core, 1] = values[t_rows:]

    def block_of(k, j):
        return hall.at[k, j, core]

    def along(k, j, way):
        block = block_of(k, j)
        return remote(block, block, z_send.at[way, k, j], h_recv.at[k, j], (down, up)[way])

    def sideways(k, j):
        block = block_of(k, j)
        return remote(block, block, x_send.at[k, j], h_recv.at[k, j], side)

    def relay(k, j):
        block = block_of(k, j)
        return remote(block, block, c_send.at[k, j], c_recv.at[k, j], partner)

    def arrived(k, j):
        sideways(k, j).wait_recv()

    def go(k, j, way):
        @pl.when((outer > 0) if way == 0 else (outer < outers - 1))
        def _():
            along(k, j, way).start()

    def doubled(k, z):
        return (k % 2 == 1) & ((z == 0) | (z == outers - 1))

    def inject(k):
        for way in range(2):
            go(k, chip, way)
        sideways(k, chip).start()
        relay(k, chip).start()

    def hop(k, r, way):
        z = outer - r if way else outer + r

        @pl.when((z >= 0) & (z < outers))
        def _():
            j = z * 2 + inner
            arrived(k, j)
            go(k, j, way)

            @pl.when(jnp.logical_not(doubled(k, z)))
            def _():
                sideways(k, j).start()

            relay(k, j).start()

    def beside(k, d):
        def one(z, way):
            @pl.when((z >= 0) & (z < outers))
            def _():
                j = z * 2 + 1 - inner
                arrived(k, j)
                if d == 0:
                    @pl.when(doubled(k, z))
                    def _():
                        for w in range(2):
                            go(k, j, w)
                else:
                    @pl.when(doubled(k, z))
                    def _():
                        go(k, j, way)

                relay(k, j).start()

        one(outer - d, 1)
        if d:
            one(outer + d, 0)

    def to_across(k):
        return remote(theirs.at[k], other.at[k], y_send.at[k], y_recv.at[k], across)

    def gather(k, d):
        def one(z):
            @pl.when((z >= 0) & (z < outers))
            def _():
                pair = (2 * z, 2 * z + 1)
                for j in pair:
                    block = hall.at[k, j, 1 - core]
                    remote(block, block, c_send.at[k, j], c_recv.at[k, j], partner).wait_recv()
                right = jnp.concatenate(
                    [jnp.concatenate([hall[k, j, c, half] for j in pair], axis=1) for half in range(2) for c in range(2)],
                    axis=0,
                )
                left = mats[:, :, pl.ds(pl.multiple_of(z * 2 * width, 128), 2 * width)].reshape(kinds * col_width, 2 * width)
                product = lax.dot_general(left, right, (((1,), (1,)), ((), ())), preferred_element_type=jnp.float32)
                acc[k] = product if d == 0 else acc[k] + product

        one(outer - d)
        if d:
            one(outer + d)

    def deliver(k):
        def lanes(half):
            return pl.ds(pl.multiple_of(half * 2 * t_rows, 128), 2 * t_rows)

        theirs[k] = acc[k, :, lanes(1 - tp)].astype(jnp.bfloat16)
        mine[k] = acc[k, :, lanes(tp)].astype(jnp.bfloat16)
        to_across(k).start()

    def conclude(k):
        to_across(k).wait_recv()

        def total(m):
            span = pl.ds(m * col_width, col_width)
            return mine[k, span, :].astype(jnp.float32) + other[k, span, :].astype(jnp.float32)

        primal = total(0)
        squashed = jax.nn.sigmoid(primal)
        squares = jnp.zeros_like(primal)
        for m in range(1, kinds):
            tangent = total(m)
            squares += tangent * tangent
        terms = squashed * (1.0 - squashed) * squares
        curves[me, pl.ds(k, 1), :] = jnp.sum(terms, axis=0, keepdims=True)
        fill = -col_width % 128
        turned = jnp.concatenate([primal, jnp.zeros((fill, 2 * t_rows), jnp.float32)], axis=0).T.astype(jnp.bfloat16)
        o, s = k // parts, k % parts
        for c in range(2):
            span = pl.ds(pl.multiple_of(((o * 2 + c) * parts + s) * t_rows, t_rows), t_rows)
            out_ref[span, :] = turned[c * t_rows : (c + 1) * t_rows, :col_width]

    lag = outers

    @pl.loop(0, count + lag)
    def _(i):
        @pl.when(i < count)
        def _():
            hidden(i)
            inject(i)

        for d in range(outers - 1):
            @pl.when((i - d - 2 >= 0) & (i - d - 2 < count))
            def _():
                gather(i - d - 2, d)

        for r in range(1, outers):
            @pl.when((i - r >= 0) & (i - r < count))
            def _():
                hop(i - r, r, 0)
                hop(i - r, r, 1)

        for d in range(outers):
            @pl.when((i - d - 1 >= 0) & (i - d - 1 < count))
            def _():
                beside(i - d - 1, d)

        @pl.when((i - lag >= 0) & (i - lag < count))
        def _():
            gather(i - lag, outers - 1)
            deliver(i - lag)

        @pl.when((i - lag - 1 >= 0) & (i - lag - 1 < count))
        def _():
            conclude(i - lag - 1)

    conclude(count - 1)

    def curve(owner, d):
        return remote(curves.at[owner], curves.at[owner], v_send.at[d], v_recv.at[owner], {"fsdp": (me + d) % devices})

    for d in range(1, devices):
        curve(me, d).start()

    def drop(a, peer):
        weight_send(a, peer).wait_send()

    for base in (chip, side_chip):
        line(base, 1, drop)
        line(base, -1, drop)
    for a in range(2):
        drop(a, side_chip)
    for copy in own_out:
        copy.wait_send()
    for a in range(2):
        for s in range(chips):
            @pl.when(s != chip)
            def _():
                weight_pass(a, s).wait_send()

    def sent(owner, way):
        for part in range(parts):
            slot = token_slot(tp, owner, part)
            remote(slot, slot, t_send.at[way, owner, part], t_recv.at[tp, owner, part], across).wait_send()

    for s in range(chips):
        sent(s, 3)
    for r in range(outers):
        @pl.when(outer - r >= 0)
        def _():
            owner = chip - 2 * r
            sent(owner, 2)

            @pl.when(outer < outers - 1)
            def _():
                sent(owner, 1)

        @pl.when(outer + r < outers)
        def _():
            owner = chip + 2 * r
            if r > 0:
                sent(owner, 2)

            @pl.when(outer > 0)
            def _():
                sent(owner, 0)

    @pl.loop(0, count)
    def _(k):
        to_across(k).wait_send()
        for j in range(chips):
            relay(k, j).wait_send()
        for z in range(outers):
            j = z * 2 + inner
            twin = z * 2 + 1 - inner
            twice = doubled(k, z)

            @pl.when((z == outer) | jnp.logical_not(twice))
            def _():
                sideways(k, j).wait_send()

            def went(way):
                along(k, j, way).wait_send()

                @pl.when(twice)
                def _():
                    along(k, twin, way).wait_send()

            @pl.when((outer <= z) & (outer > 0))
            def _():
                went(0)

            @pl.when((outer >= z) & (outer < outers - 1))
            def _():
                went(1)

    for d in range(1, devices):
        curve((me + devices - d) % devices, d).wait_recv()
        curve(me, d).wait_send()
    totals = jnp.sum(curves[...], axis=0) / (PROBES * D)
    for o in range(owners):
        for c in range(2):
            row = [totals[o * parts + s : o * parts + s + 1, c * t_rows : (c + 1) * t_rows] for s in range(parts)]
            curv_ref[pl.ds(o * 2 + c, 1), :] = jnp.concatenate(row, axis=1)


def fused(tokens, norm_gain, gate_weight, up_weight, down_weight, probes, chips):
    t_all, t_cols = tokens.shape
    parts = 2 if t_all % 128 == 0 else 1
    t_rows = t_all // parts
    rows, columns = gate_weight.shape
    width = columns // chips
    col_width, span = down_weight.shape
    kinds = 1 + probes.shape[0]
    count = parts * chips // 2
    kept = count * 2 * t_rows
    pieces = pltpu.SemaphoreType.DMA((2, chips))
    hops = pltpu.SemaphoreType.DMA((count, chips))
    part = pltpu.VMEM((count, kinds * col_width, 2 * t_rows), jnp.bfloat16)
    vmem = pl.BlockSpec(memory_space=pltpu.VMEM)
    out, curv = pl.pallas_call(
        lambda *refs: fused_kernel(chips, *refs),
        out_shape=(jax.ShapeDtypeStruct((kept, col_width), jnp.bfloat16), jax.ShapeDtypeStruct((chips, t_all), jnp.float32)),
        in_specs=[ANY, vmem, ANY, ANY, ANY, ANY],
        out_specs=[vmem] * 2,
        scratch_shapes=[
            pltpu.VMEM((chips, parts, t_rows, 2 * t_cols), jnp.bfloat16),
            pltpu.VMEM((chips, 2, rows, 2 * width), jnp.bfloat16),
            pltpu.VMEM((count, chips, 2, 2, t_rows, width), jnp.bfloat16),
            pltpu.VMEM((kinds, col_width, span), jnp.bfloat16),
            pltpu.VMEM((count, kinds * col_width, 4 * t_rows), jnp.float32),
            part,
            part,
            part,
            pltpu.VMEM((2 * chips, count, 2 * t_rows), jnp.float32),
            pltpu.SemaphoreType.DMA((4, chips, parts)),
            pltpu.SemaphoreType.DMA((2, chips, parts)),
            pieces,
            pieces,
            pieces,
            pieces,
            pltpu.SemaphoreType.DMA((2, count, chips)),
            hops,
            hops,
            hops,
            hops,
            pltpu.SemaphoreType.DMA((count,)),
            pltpu.SemaphoreType.DMA((count,)),
            pltpu.SemaphoreType.DMA((2 * chips,)),
            pltpu.SemaphoreType.DMA((2 * chips,)),
            pltpu.SemaphoreType.DMA((5,)),
        ],
        compiler_params=pltpu.CompilerParams(collective_id=1, has_side_effects=True, vmem_limit_bytes=63 * 2**20),
        name="fused",
    )(tokens.reshape(parts, t_rows, t_cols), norm_gain, gate_weight, up_weight, down_weight, probes)
    return out, curv.reshape(kept)


def norm(features, norm_gain):
    widened = features.astype(jnp.float32)
    inverse_rms = lax.rsqrt(jnp.mean(widened * widened, axis=1, keepdims=True) + epsilon)
    return (widened * inverse_rms * norm_gain.astype(jnp.float32)).astype(jnp.bfloat16)


def dot(a, b):
    return jnp.dot(a, b, preferred_element_type=jnp.float32)


def project(hidden_all, down_weight, probes):
    stacked = jnp.concatenate([down_weight[None], probes], axis=0)
    count = stacked.shape[0]
    col_width = stacked.shape[1]
    flat_weights = stacked.reshape(count * col_width, stacked.shape[2])
    partial_terms = lax.dot_general(
        hidden_all,
        flat_weights,
        (((1,), (1,)), ((), ())),
        preferred_element_type=jnp.float32,
    )
    summed = lax.psum_scatter(
        partial_terms.astype(jnp.bfloat16), "tp", scatter_dimension=0, tiled=True
    ).astype(jnp.float32)
    summed_parts = summed.reshape(summed.shape[0], count, col_width)
    primal = summed_parts[:, 0, :]
    tangents = summed_parts[:, 1:, :]
    squashed = jax.nn.sigmoid(primal)
    slope = squashed * (1.0 - squashed)
    tangent_sq = jnp.sum(tangents * tangents, axis=1)
    local_curv = jnp.sum(slope * tangent_sq, axis=1) / (PROBES * D)
    token_curv = lax.psum(local_curv, "fsdp")
    return (primal.astype(jnp.bfloat16), token_curv)


def gathered_weights(tokens, norm_gain, gate_weight, up_weight, down_weight, probes):
    normed = norm(lax.all_gather(tokens, "tp", axis=1, tiled=True), norm_gain)
    gate_sum = dot(normed, lax.all_gather(gate_weight, "fsdp", axis=0, tiled=True))
    up_sum = dot(normed, lax.all_gather(up_weight, "fsdp", axis=0, tiled=True))
    hidden = (jax.nn.silu(gate_sum) * up_sum).astype(jnp.bfloat16)
    return project(lax.all_gather(hidden, "fsdp", axis=0, tiled=True), down_weight, probes)


def moved_weights(tokens, norm_gain, gate_weight, up_weight, down_weight, probes):
    chips = lax.axis_size("fsdp") // 2
    return fused(tokens, norm_gain, gate_weight, up_weight, down_weight, probes, chips)


def solution(mesh):
    def on_device(tokens, norm_gain, gate_weight, up_weight, down_weight, probes):
        chips = mesh.shape["fsdp"] // 2
        fits = mesh.shape["tp"] == 2 and chips % 2 == 0 and gate_weight.shape[1] % (128 * chips) == 0 and tokens.shape[1] % 128 == 0
        form = moved_weights if fits else gathered_weights
        return form(tokens, norm_gain, gate_weight, up_weight, down_weight, probes)

    return jax.shard_map(
        on_device,
        mesh=mesh,
        in_specs=(
            P("fsdp", "tp"),
            P(),
            P("fsdp", "tp"),
            P("fsdp", "tp"),
            P("fsdp", "tp"),
            P(None, "fsdp", "tp"),
        ),
        out_specs=(P("tp", "fsdp"), P("tp")),
        check_vma=False,
    )
```

```python
import jax
import jax.numpy as jnp
from jax import lax
from jax.experimental import pallas as pl
from jax.experimental.pallas import tpu as pltpu
from jax.sharding import PartitionSpec as P

D = 3584
PROBES = 2
MESH = pl.DeviceIdType.MESH
ANY = pl.BlockSpec(memory_space=pl.ANY)


epsilon = 1e-06


def remote(src, dst, send, recv, device):
    return pltpu.make_async_remote_copy(
        src_ref=src,
        dst_ref=dst,
        send_sem=send,
        recv_sem=recv,
        device_id=device,
        device_id_type=MESH,
    )


def fused_kernel(chips, t_ref, gain_ref, g_ref, u_ref, m0_ref, mp_ref, out_ref, curv_ref, tok, wts, hall, mats, acc, mine, theirs, other, curves,
                 t_send, t_recv, w_send, w_recv, wc_send, wc_recv, z_send, x_send, h_recv, c_send, c_recv, y_send, y_recv, v_send, v_recv, local_sem):
    me = lax.axis_index("fsdp")
    tp = lax.axis_index("tp")
    chip, core = me // 2, me % 2
    outer, inner = chip // 2, chip % 2
    outers = chips // 2
    devices = 2 * chips
    owners = chips // 2
    parts, t_rows, t_cols = t_ref.shape
    rows = g_ref.shape[0]
    count = hall.shape[0]
    width = hall.shape[-1]
    kinds, col_width = 1 + mp_ref.shape[0], m0_ref.shape[0]
    side_chip = outer * 2 + 1 - inner
    partner = {"fsdp": chip * 2 + 1 - core}
    across = {"tp": 1 - tp}
    down = {"fsdp": (chip - 2) * 2 + core}
    up = {"fsdp": (chip + 2) * 2 + core}
    side = {"fsdp": side_chip * 2 + core}
    features = chips * 2 * rows

    barrier = pltpu.get_barrier_semaphore()
    for d in range(1, devices):
        pl.semaphore_signal(barrier, inc=1, device_id={"fsdp": (me + d) % devices}, device_id_type=MESH)
    pl.semaphore_signal(barrier, inc=1, device_id=across, device_id_type=MESH)
    pl.semaphore_wait(barrier, devices)

    def token_slot(half, owner, part):
        return tok.at[owner, part, :, pl.ds(pl.multiple_of(half * t_cols, 128), t_cols)]

    def token_copy(src, half, owner, part, way, device):
        return remote(src, token_slot(half, owner, part), t_send.at[way, owner, part], t_recv.at[half, owner, part], device)

    def pass_on(src, owner, part, first):
        if first in (0, 1):
            @pl.when(outer > 0)
            def _():
                token_copy(src, tp, owner, part, 0, down).start()
        if first in (0, 2):
            @pl.when(outer < outers - 1)
            def _():
                token_copy(src, tp, owner, part, 1, up).start()
        token_copy(src, tp, owner, part, 2, side).start()
        token_copy(src, tp, owner, part, 3, across).start()

    def token_wait(half, owner, part):
        slot = token_slot(half, owner, part)
        remote(slot, slot, t_send.at[3, owner, part], t_recv.at[half, owner, part], across).wait_recv()

    weights = (g_ref, u_ref)

    def piece(a, owner):
        return weights[a].at[:, pl.ds(pl.multiple_of(owner * width, 128), width)]

    def landing(a, source, c):
        return wts.at[source, c, :, pl.ds(a * width, width)]

    def weight_send(a, peer):
        return remote(piece(a, peer), landing(a, chip, core), w_send.at[a, peer], w_recv.at[a, chip], {"fsdp": peer * 2 + core})

    def weight_pass(a, source):
        block = landing(a, source, core)
        return remote(block, block, wc_send.at[a, source], wc_recv.at[a, source], partner)

    def line(base, step, act):
        for d in range(outers - 1, 0, -1):
            @pl.when((outer + step * d >= 0) & (outer + step * d < outers))
            def _():
                for a in range(2):
                    act(a, base + 2 * step * d)

    def start_send(a, peer):
        weight_send(a, peer).start()

    def weights_along(r):
        @pl.when(outer == r)
        def _():
            line(chip, 1, start_send)
            line(side_chip, 1, start_send)

        @pl.when(outer == outers - 1 - r)
        def _():
            line(chip, -1, start_send)
            line(side_chip, -1, start_send)

    for part in range(parts):
        pass_on(t_ref.at[part], chip, part, 0)
    for a in range(2):
        start_send(a, side_chip)
    weights_along(0)
    own_out = [remote(piece(a, chip), landing(a, chip, core), wc_send.at[a, chip], wc_recv.at[a, chip], partner) for a in range(2)]
    locals_ = [pltpu.make_async_copy(piece(a, chip), landing(a, chip, core), local_sem.at[a]) for a in range(2)]
    locals_ += [
        pltpu.make_async_copy(t_ref, tok.at[chip, :, :, pl.ds(pl.multiple_of(tp * t_cols, 128), t_cols)], local_sem.at[2]),
        pltpu.make_async_copy(m0_ref, mats.at[0], local_sem.at[3]),
        pltpu.make_async_copy(mp_ref, mats.at[pl.ds(1, kinds - 1)], local_sem.at[4]),
    ]
    for copy in own_out + locals_:
        copy.start()

    for r in range(1, outers):
        @pl.when(outer - r >= 0)
        def _():
            owner = chip - 2 * r
            for part in range(parts):
                token_wait(tp, owner, part)
                pass_on(token_slot(tp, owner, part), owner, part, 2)

        @pl.when(outer + r < outers)
        def _():
            owner = chip + 2 * r
            for part in range(parts):
                token_wait(tp, owner, part)
                pass_on(token_slot(tp, owner, part), owner, part, 1)

        weights_along(r)

    for z in range(outers):
        owner = z * 2 + 1 - inner
        for part in range(parts):
            token_wait(tp, owner, part)
            token_copy(token_slot(tp, owner, part), tp, owner, part, 3, across).start()

    def take(a, source):
        block = landing(a, source, core)
        remote(block, block, w_send.at[a, source], w_recv.at[a, source], partner).wait_recv()
        weight_pass(a, source).start()

    line(chip, 1, take)
    line(chip, -1, take)
    for a in range(2):
        take(a, side_chip)
    line(side_chip, 1, take)
    line(side_chip, -1, take)
    for s in range(chips):
        for a in range(2):
            block = landing(a, s, 1 - core)
            remote(block, block, wc_send.at[a, s], wc_recv.at[a, s], partner).wait_recv()
    for copy in locals_:
        copy.wait()

    def hidden(k):
        o, s = k // parts, k % parts

        for half in range(2):
            token_wait(1 - tp, half * owners + o, s)

        def normed(owner):
            widened = tok[owner, s].astype(jnp.float32)
            inverse_rms = lax.rsqrt(jnp.mean(widened * widened, axis=1, keepdims=True) + epsilon)
            return (widened * inverse_rms * gain_ref[...].astype(jnp.float32)[None, :]).astype(jnp.bfloat16)

        left = jnp.concatenate([normed(o), normed(owners + o)], axis=0)
        sums = jnp.dot(left, wts[...].reshape(features, 2 * width), preferred_element_type=jnp.float32)
        values = (jax.nn.silu(sums[:, :width]) * sums[:, width:]).astype(jnp.bfloat16)
        hall[k, chip, core, 0] = values[:t_rows]
        hall[k, chip, core, 1] = values[t_rows:]

    def block_of(k, j):
        return hall.at[k, j, core]

    def along(k, j, way):
        block = block_of(k, j)
        return remote(block, block, z_send.at[way, k, j], h_recv.at[k, j], (down, up)[way])

    def sideways(k, j):
        block = block_of(k, j)
        return remote(block, block, x_send.at[k, j], h_recv.at[k, j], side)

    def relay(k, j):
        block = block_of(k, j)
        return remote(block, block, c_send.at[k, j], c_recv.at[k, j], partner)

    def arrived(k, j):
        sideways(k, j).wait_recv()

    def go(k, j, way):
        @pl.when((outer > 0) if way == 0 else (outer < outers - 1))
        def _():
            along(k, j, way).start()

    def doubled(k, z):
        return (k % 2 == 1) & ((z == 0) | (z == outers - 1))

    def inject(k):
        for way in range(2):
            go(k, chip, way)
        sideways(k, chip).start()
        relay(k, chip).start()

    def hop(k, r, way):
        z = outer - r if way else outer + r

        @pl.when((z >= 0) & (z < outers))
        def _():
            j = z * 2 + inner
            arrived(k, j)
            go(k, j, way)

            @pl.when(jnp.logical_not(doubled(k, z)))
            def _():
                sideways(k, j).start()

            relay(k, j).start()

    def beside(k, d):
        def one(z, way):
            @pl.when((z >= 0) & (z < outers))
            def _():
                j = z * 2 + 1 - inner
                arrived(k, j)
                if d == 0:
                    @pl.when(doubled(k, z))
                    def _():
                        for w in range(2):
                            go(k, j, w)
                else:
                    @pl.when(doubled(k, z))
                    def _():
                        go(k, j, way)

                relay(k, j).start()

        one(outer - d, 1)
        if d:
            one(outer + d, 0)

    def to_across(k):
        return remote(theirs.at[k], other.at[k], y_send.at[k], y_recv.at[k], across)

    def gather(k, d):
        def one(z):
            @pl.when((z >= 0) & (z < outers))
            def _():
                pair = (2 * z, 2 * z + 1)
                for j in pair:
                    block = hall.at[k, j, 1 - core]
                    remote(block, block, c_send.at[k, j], c_recv.at[k, j], partner).wait_recv()
                right = jnp.concatenate(
                    [jnp.concatenate([hall[k, j, c, half] for j in pair], axis=1) for half in range(2) for c in range(2)],
                    axis=0,
                )
                left = mats[:, :, pl.ds(pl.multiple_of(z * 2 * width, 128), 2 * width)].reshape(kinds * col_width, 2 * width)
                product = lax.dot_general(left, right, (((1,), (1,)), ((), ())), preferred_element_type=jnp.float32)
                acc[k] = product if d == 0 else acc[k] + product

        one(outer - d)
        if d:
            one(outer + d)

    def deliver(k):
        def lanes(half):
            return pl.ds(pl.multiple_of(half * 2 * t_rows, 128), 2 * t_rows)

        theirs[k] = acc[k, :, lanes(1 - tp)].astype(jnp.bfloat16)
        mine[k] = acc[k, :, lanes(tp)].astype(jnp.bfloat16)
        to_across(k).start()

    def conclude(k):
        to_across(k).wait_recv()

        def total(m):
            span = pl.ds(m * col_width, col_width)
            return mine[k, span, :].astype(jnp.float32) + other[k, span, :].astype(jnp.float32)

        primal = total(0)
        squashed = jax.nn.sigmoid(primal)
        squares = jnp.zeros_like(primal)
        for m in range(1, kinds):
            tangent = total(m)
            squares += tangent * tangent
        terms = squashed * (1.0 - squashed) * squares
        curves[me, pl.ds(k, 1), :] = jnp.sum(terms, axis=0, keepdims=True)
        fill = -col_width % 128
        turned = jnp.concatenate([primal, jnp.zeros((fill, 2 * t_rows), jnp.float32)], axis=0).T.astype(jnp.bfloat16)
        o, s = k // parts, k % parts
        for c in range(2):
            span = pl.ds(pl.multiple_of(((o * 2 + c) * parts + s) * t_rows, t_rows), t_rows)
            out_ref[span, :] = turned[c * t_rows : (c + 1) * t_rows, :col_width]

    lag = outers + 1

    @pl.loop(0, count + lag)
    def _(i):
        @pl.when(i < count)
        def _():
            hidden(i)
            inject(i)

        for d in range(outers - 1):
            @pl.when((i - d - 3 >= 0) & (i - d - 3 < count))
            def _():
                gather(i - d - 3, d)

        for r in range(1, outers):
            @pl.when((i - r - 1 >= 0) & (i - r - 1 < count))
            def _():
                hop(i - r - 1, r, 0)
                hop(i - r - 1, r, 1)

        for d in range(outers):
            @pl.when((i - d - 2 >= 0) & (i - d - 2 < count))
            def _():
                beside(i - d - 2, d)

        @pl.when((i - lag >= 0) & (i - lag < count))
        def _():
            gather(i - lag, outers - 1)
            deliver(i - lag)

        @pl.when((i - lag - 1 >= 0) & (i - lag - 1 < count))
        def _():
            conclude(i - lag - 1)

    conclude(count - 1)

    def curve(owner, d):
        return remote(curves.at[owner], curves.at[owner], v_send.at[d], v_recv.at[owner], {"fsdp": (me + d) % devices})

    for d in range(1, devices):
        curve(me, d).start()

    def drop(a, peer):
        weight_send(a, peer).wait_send()

    for base in (chip, side_chip):
        line(base, 1, drop)
        line(base, -1, drop)
    for a in range(2):
        drop(a, side_chip)
    for copy in own_out:
        copy.wait_send()
    for a in range(2):
        for s in range(chips):
            @pl.when(s != chip)
            def _():
                weight_pass(a, s).wait_send()

    def sent(owner, way):
        for part in range(parts):
            slot = token_slot(tp, owner, part)
            remote(slot, slot, t_send.at[way, owner, part], t_recv.at[tp, owner, part], across).wait_send()

    for s in range(chips):
        sent(s, 3)
    for r in range(outers):
        @pl.when(outer - r >= 0)
        def _():
            owner = chip - 2 * r
            sent(owner, 2)

            @pl.when(outer < outers - 1)
            def _():
                sent(owner, 1)

        @pl.when(outer + r < outers)
        def _():
            owner = chip + 2 * r
            if r > 0:
                sent(owner, 2)

            @pl.when(outer > 0)
            def _():
                sent(owner, 0)

    @pl.loop(0, count)
    def _(k):
        to_across(k).wait_send()
        for j in range(chips):
            relay(k, j).wait_send()
        for z in range(outers):
            j = z * 2 + inner
            twin = z * 2 + 1 - inner
            twice = doubled(k, z)

            @pl.when((z == outer) | jnp.logical_not(twice))
            def _():
                sideways(k, j).wait_send()

            def went(way):
                along(k, j, way).wait_send()

                @pl.when(twice)
                def _():
                    along(k, twin, way).wait_send()

            @pl.when((outer <= z) & (outer > 0))
            def _():
                went(0)

            @pl.when((outer >= z) & (outer < outers - 1))
            def _():
                went(1)

    for d in range(1, devices):
        curve((me + devices - d) % devices, d).wait_recv()
        curve(me, d).wait_send()
    totals = jnp.sum(curves[...], axis=0) / (PROBES * D)
    for o in range(owners):
        for c in range(2):
            row = [totals[o * parts + s : o * parts + s + 1, c * t_rows : (c + 1) * t_rows] for s in range(parts)]
            curv_ref[pl.ds(o * 2 + c, 1), :] = jnp.concatenate(row, axis=1)


def fused(tokens, norm_gain, gate_weight, up_weight, down_weight, probes, chips):
    t_all, t_cols = tokens.shape
    parts = 2 if t_all % 128 == 0 else 1
    t_rows = t_all // parts
    rows, columns = gate_weight.shape
    width = columns // chips
    col_width, span = down_weight.shape
    kinds = 1 + probes.shape[0]
    count = parts * chips // 2
    kept = count * 2 * t_rows
    pieces = pltpu.SemaphoreType.DMA((2, chips))
    hops = pltpu.SemaphoreType.DMA((count, chips))
    part = pltpu.VMEM((count, kinds * col_width, 2 * t_rows), jnp.bfloat16)
    vmem = pl.BlockSpec(memory_space=pltpu.VMEM)
    out, curv = pl.pallas_call(
        lambda *refs: fused_kernel(chips, *refs),
        out_shape=(jax.ShapeDtypeStruct((kept, col_width), jnp.bfloat16), jax.ShapeDtypeStruct((chips, t_all), jnp.float32)),
        in_specs=[ANY, vmem, ANY, ANY, ANY, ANY],
        out_specs=[vmem] * 2,
        scratch_shapes=[
            pltpu.VMEM((chips, parts, t_rows, 2 * t_cols), jnp.bfloat16),
            pltpu.VMEM((chips, 2, rows, 2 * width), jnp.bfloat16),
            pltpu.VMEM((count, chips, 2, 2, t_rows, width), jnp.bfloat16),
            pltpu.VMEM((kinds, col_width, span), jnp.bfloat16),
            pltpu.VMEM((count, kinds * col_width, 4 * t_rows), jnp.float32),
            part,
            part,
            part,
            pltpu.VMEM((2 * chips, count, 2 * t_rows), jnp.float32),
            pltpu.SemaphoreType.DMA((4, chips, parts)),
            pltpu.SemaphoreType.DMA((2, chips, parts)),
            pieces,
            pieces,
            pieces,
            pieces,
            pltpu.SemaphoreType.DMA((2, count, chips)),
            hops,
            hops,
            hops,
            hops,
            pltpu.SemaphoreType.DMA((count,)),
            pltpu.SemaphoreType.DMA((count,)),
            pltpu.SemaphoreType.DMA((2 * chips,)),
            pltpu.SemaphoreType.DMA((2 * chips,)),
            pltpu.SemaphoreType.DMA((5,)),
        ],
        compiler_params=pltpu.CompilerParams(collective_id=1, has_side_effects=True, vmem_limit_bytes=63 * 2**20),
        name="fused",
    )(tokens.reshape(parts, t_rows, t_cols), norm_gain, gate_weight, up_weight, down_weight, probes)
    return out, curv.reshape(kept)


def norm(features, norm_gain):
    widened = features.astype(jnp.float32)
    inverse_rms = lax.rsqrt(jnp.mean(widened * widened, axis=1, keepdims=True) + epsilon)
    return (widened * inverse_rms * norm_gain.astype(jnp.float32)).astype(jnp.bfloat16)


def dot(a, b):
    return jnp.dot(a, b, preferred_element_type=jnp.float32)


def project(hidden_all, down_weight, probes):
    stacked = jnp.concatenate([down_weight[None], probes], axis=0)
    count = stacked.shape[0]
    col_width = stacked.shape[1]
    flat_weights = stacked.reshape(count * col_width, stacked.shape[2])
    partial_terms = lax.dot_general(
        hidden_all,
        flat_weights,
        (((1,), (1,)), ((), ())),
        preferred_element_type=jnp.float32,
    )
    summed = lax.psum_scatter(
        partial_terms.astype(jnp.bfloat16), "tp", scatter_dimension=0, tiled=True
    ).astype(jnp.float32)
    summed_parts = summed.reshape(summed.shape[0], count, col_width)
    primal = summed_parts[:, 0, :]
    tangents = summed_parts[:, 1:, :]
    squashed = jax.nn.sigmoid(primal)
    slope = squashed * (1.0 - squashed)
    tangent_sq = jnp.sum(tangents * tangents, axis=1)
    local_curv = jnp.sum(slope * tangent_sq, axis=1) / (PROBES * D)
    token_curv = lax.psum(local_curv, "fsdp")
    return (primal.astype(jnp.bfloat16), token_curv)


def gathered_weights(tokens, norm_gain, gate_weight, up_weight, down_weight, probes):
    normed = norm(lax.all_gather(tokens, "tp", axis=1, tiled=True), norm_gain)
    gate_sum = dot(normed, lax.all_gather(gate_weight, "fsdp", axis=0, tiled=True))
    up_sum = dot(normed, lax.all_gather(up_weight, "fsdp", axis=0, tiled=True))
    hidden = (jax.nn.silu(gate_sum) * up_sum).astype(jnp.bfloat16)
    return project(lax.all_gather(hidden, "fsdp", axis=0, tiled=True), down_weight, probes)


def moved_weights(tokens, norm_gain, gate_weight, up_weight, down_weight, probes):
    chips = lax.axis_size("fsdp") // 2
    return fused(tokens, norm_gain, gate_weight, up_weight, down_weight, probes, chips)


def solution(mesh):
    def on_device(tokens, norm_gain, gate_weight, up_weight, down_weight, probes):
        chips = mesh.shape["fsdp"] // 2
        fits = mesh.shape["tp"] == 2 and chips % 2 == 0 and gate_weight.shape[1] % (128 * chips) == 0 and tokens.shape[1] % 128 == 0
        form = moved_weights if fits else gathered_weights
        return form(tokens, norm_gain, gate_weight, up_weight, down_weight, probes)

    return jax.shard_map(
        on_device,
        mesh=mesh,
        in_specs=(
            P("fsdp", "tp"),
            P(),
            P("fsdp", "tp"),
            P("fsdp", "tp"),
            P("fsdp", "tp"),
            P(None, "fsdp", "tp"),
        ),
        out_specs=(P("tp", "fsdp"), P("tp")),
        check_vma=False,
    )
```
